32 devices in a mesh: cluster: 8 (over z, y), sub: 4 (over x, core).
Axes of the slice: x: 2, y: 2, z: 4, core: 2. Of those that a mesh axis runs over, the one named last changes fastest.
Arguments:
- right_side: float32 [4, 8, 16, 384], P('sub', 'cluster'), may hold values from -12 to 12
- schur: float32 [4, 8, 768, 768], P('sub', 'cluster'), as said below
- rigid_modes: float32 [4, 8, 6, 768], P('sub', 'cluster'), may hold values from -0.21875 to 0.21875
- mode_count: int32 [4, 8], P('sub', 'cluster'), may hold values from 3 to 6
- face_order: int32 [4, 8, 384], P('sub', 'cluster'), may hold values from 0 to 383, each once within a row
- dual_scale: float32 [4, 8, 384], P('sub', 'cluster'), may hold values from 0.5 to 2
- rigid_loads: float32 [4, 8, 6, 16], P('sub', 'cluster'), may hold values from -6 to 6
- coarse_inverse: float32 [192, 192], P(('cluster', 'sub')), as said below
Outputs:
- multipliers: float32 [4, 8, 16, 384], P('sub', 'cluster')
- residual: float32 [4, 8, 16, 384], P('sub', 'cluster')
The draws below stay inside these ranges and needn't reach their ends.
Inputs may be any that keep to these rules, and one draw needn't show every extreme that they name: rigid-body modes m with m >= mode_count are unused. `face_order`: each subdomain's entries form a permutation of the face unknowns; those of the first subdomain of a chain are unused. `schur`: each subdomain's matrix is symmetric. `coarse_inverse`: symmetric.
All inputs are finite; a program needn't handle non-finite values.
Results may differ from the reference program's by a relative error of at most 0.0003.
Values sent between devices are 32-bit elements; how exact they have to be, the bound alone decides.
No kernel may reach another device: no remote copies, remote signals or barrier semaphores. Data moves between devices by JAX's collectives and lax.ppermute only.
A program may use at most 64 MiB of HBM per device.

```python
import math
import jax
import jax.numpy as jnp
from jax import lax

NI = 768
M = 384
CASES = 16
MODES = 6
ITERS = 2
SUB_DEV = 1
CHAIN = 8
NC = 192
N_CLUSTER = 8
N_SUB = 4


def draw_schur(key, part):

    def single_matrix(matrix_index):
        sub_key = jax.random.fold_in(key, matrix_index)
        random_part = jax.random.normal(sub_key, (NI, NI), jnp.float32)
        symmetric = (random_part + random_part.T) * (0.5 / jnp.sqrt(2.0 * NI))
        return symmetric + 2.0 * jnp.eye(NI, dtype=jnp.float32)
    matrices = lax.map(single_matrix, jnp.arange(N_SUB * CHAIN))
    return matrices.reshape(N_SUB, CHAIN, NI, NI)


def draw_coarse_inverse(key, part):
    random_part = jax.random.normal(key, (NC, NC), jnp.float32)
    return jnp.eye(NC, dtype=jnp.float32) + (random_part + random_part.T) * (0.5 / jnp.sqrt(2.0 * NC))


def draw_right_side(key, part):
    growth = 1.0 + 2.0 * jnp.arange(CHAIN, dtype=jnp.float32) / max(CHAIN - 1, 1)
    growth = growth[None, :, None, None]
    random_part = jnp.clip(jax.random.normal(key, (N_SUB, CHAIN, CASES, M), jnp.float32), -4.0, 4.0)
    return random_part * growth


def plant(values, stream_key, smallest, largest):
    extent = values.shape
    index_at = [jax.random.randint(jax.random.fold_in(stream_key, axis), (), 0, extent[axis]) for axis in range(len(extent))]
    values = values.at[tuple(index_at)].set(smallest)
    longest = extent.index(max(extent))
    index_at[longest] = (index_at[longest] + 1) % extent[longest]
    return values.at[tuple(index_at)].set(largest)


def block_scale(own_key, dims, pieces, low, high):
    def one(position, blocks):
        steps = jax.random.uniform(jax.random.fold_in(jax.random.fold_in(own_key, 6), position), (blocks,), jnp.float32, low / len(pieces), high / len(pieces))
        return jnp.repeat(jnp.exp(steps), dims[position] // blocks).reshape((-1,) + (1,) * (len(dims) - position - 1))

    loudness = one(*pieces[0])
    for cut in pieces[1:]:
        loudness = loudness * one(*cut)
    return loudness


def centred(stream_key, dims, deviation, bound, shards=(), kind=jnp.bfloat16):
    loudness = block_scale(stream_key, dims, shards, -0.22, 0.18) if shards else 1.0
    drawn = jax.random.normal(stream_key, dims, jnp.float32) * deviation * loudness
    return jnp.minimum(jnp.maximum(drawn, -bound), bound).astype(kind)


def setup_inputs(seed: int = 0) -> dict:
    arg_keys = jax.random.split(jax.random.key(seed), 9)
    return {
        "right_side": draw_right_side(jax.random.fold_in(arg_keys[8], 71), 0),
        "schur": draw_schur(jax.random.fold_in(arg_keys[8], 71), 0),
        "rigid_modes": centred(arg_keys[2], (N_SUB, CHAIN, MODES, NI), NI ** -0.5, 0.21875, ((0, 4), (1, 8)), jnp.float32),
        "mode_count": plant(jax.random.randint(arg_keys[3], (N_SUB, CHAIN), 3, 7), jax.random.fold_in(arg_keys[3], 1), 3, 6).astype(jnp.int32),
        "face_order": jax.vmap(lambda own: jax.random.permutation(own, M))(jax.random.split(arg_keys[4], N_SUB * CHAIN)).reshape((N_SUB, CHAIN, M)).astype(jnp.int32),
        "dual_scale": jnp.clip(jnp.exp(math.log(2.0) - 1.3862944 * jax.random.uniform(arg_keys[5], (N_SUB, CHAIN, M), jnp.float32) ** block_scale(arg_keys[5], (N_SUB, CHAIN, M), ((0, 4), (1, 8)), -0.2, 0.2)), 0.5, 2.0),
        "rigid_loads": centred(arg_keys[6], (N_SUB, CHAIN, MODES, CASES), 1.0, 6.0, ((0, 4), (1, 8)), jnp.float32),
        "coarse_inverse": draw_coarse_inverse(jax.random.fold_in(arg_keys[8], 71), 0),
    }


highest = lax.Precision.HIGHEST

def lift_faces(dual_field, face_order):
    earlier = jnp.concatenate([jnp.zeros_like(dual_field[:, :1]), dual_field[:, :-1]], axis=1)
    gather_index = jnp.broadcast_to(face_order[:, :, None, :], earlier.shape)
    left_face = -jnp.take_along_axis(earlier, gather_index, axis=3)
    return jnp.concatenate([left_face, dual_field], axis=3)

def push_faces(values, inverse):
    half_size = values.shape[3] // 2
    left_face = values[..., :half_size]
    right_face = values[..., half_size:]
    gather_index = jnp.broadcast_to(inverse[:, :, None, :], left_face.shape)
    returned = -jnp.take_along_axis(left_face, gather_index, axis=3)
    following = jnp.concatenate([returned[:, 1:], jnp.zeros_like(returned[:, :1])], axis=1)
    return right_face + following

def apply_dual(dual_field, schur, face_order, inverse):
    lifted = lift_faces(dual_field, face_order)
    dual_image = jnp.einsum('sjci,sjik->sjck', lifted, schur, precision=highest)
    return push_faces(dual_image, inverse)

def basis_transpose(dual_field, basis, face_order):
    return jnp.einsum('sjmi,sjci->sjmc', basis, lift_faces(dual_field, face_order), precision=highest)

def basis_expand(coefficients, basis, inverse):
    return push_faces(jnp.einsum('sjmi,sjmc->sjci', basis, coefficients, precision=highest), inverse)

def coarse_solve(coefficients, coarse_inverse):
    flattened = coefficients.reshape(N_SUB, N_CLUSTER, SUB_DEV, MODES, CASES).transpose(1, 0, 2, 3, 4).reshape(NC, CASES)
    solved = jnp.dot(coarse_inverse, flattened, precision=highest)
    return solved.reshape(N_CLUSTER, N_SUB, SUB_DEV, MODES, CASES).transpose(1, 0, 2, 3, 4).reshape(N_SUB, CHAIN, MODES, CASES)

def project(dual_field, basis, face_order, inverse, coarse_inverse):
    coefficients = basis_transpose(dual_field, basis, face_order)
    return dual_field - basis_expand(coarse_solve(coefficients, coarse_inverse), basis, inverse)

def gram_product(first_field, second_field):
    return jnp.einsum('sjcm,sjdm->cd', first_field, second_field, precision=highest)

def solve_small(matrix, right_hand):
    factor = jnp.linalg.cholesky(matrix)
    halfway = lax.linalg.triangular_solve(factor, right_hand, left_side=True, lower=True)
    return lax.linalg.triangular_solve(factor, halfway, left_side=True, lower=True, transpose_a=True)

def reference(right_side, schur, rigid_modes, mode_count, face_order, dual_scale, rigid_loads, coarse_inverse):
    inverse = jnp.argsort(face_order, axis=-1).astype(jnp.int32)
    active = (jnp.arange(MODES)[None, None, :] < mode_count[:, :, None]).astype(jnp.float32)
    basis = rigid_modes * active[..., None]
    masked_loads = rigid_loads * active[..., None]
    scaling = dual_scale[:, :, None, :]
    multipliers = basis_expand(coarse_solve(masked_loads, coarse_inverse), basis, inverse)
    residual = project(right_side - apply_dual(multipliers, schur, face_order, inverse), basis, face_order, inverse, coarse_inverse)
    search = project(scaling * residual, basis, face_order, inverse, coarse_inverse)
    direction = search
    for iteration in range(ITERS):
        dual_image = apply_dual(direction, schur, face_order, inverse)
        curvature = gram_product(direction, dual_image)
        descent = gram_product(direction, residual)
        projected_image = project(dual_image, basis, face_order, inverse, coarse_inverse)
        step_size = solve_small(curvature, descent)
        multipliers = multipliers + jnp.einsum('sjcm,cd->sjdm', direction, step_size, precision=highest)
        residual = residual - jnp.einsum('sjcm,cd->sjdm', projected_image, step_size, precision=highest)
        if iteration + 1 < ITERS:
            search = project(scaling * residual, basis, face_order, inverse, coarse_inverse)
            correction = -solve_small(curvature, gram_product(dual_image, search))
            direction = search + jnp.einsum('sjcm,cd->sjdm', direction, correction, precision=highest)
    return (multipliers, residual)
```

```python
import functools
import jax
import jax.numpy as jnp
from jax import lax
from jax.experimental import pallas as pl
from jax.experimental.pallas import tpu as pltpu
from jax.sharding import PartitionSpec as P

AXES = ("cluster", "sub")
f32 = jnp.float32
bf16 = jnp.bfloat16
PAD = 8


def dot(a, b, ca, cb):
    return lax.dot_general(
        a, b, (((ca,), (cb,)), ((), ())), precision=lax.Precision.HIGHEST, preferred_element_type=f32
    )


def nn(a, b):
    return dot(a, b, 1, 0)


def nt(a, b):
    return dot(a, b, 1, 1)


def tn(a, b):
    return dot(a, b, 0, 0)


def bdot(a, b, ca, cb):
    return lax.dot_general(a, b, (((ca,), (cb,)), ((), ())), preferred_element_type=f32)


def halves(x):
    high = x.astype(bf16)
    return high, (x - high.astype(f32)).astype(bf16)


def times_schur(x, high_ref, low_ref):
    rows = x.shape[0]
    xh, xl = halves(x)
    both = bdot(jnp.concatenate([xh, xl], axis=0), high_ref[...], 1, 0)
    return both[:rows] + both[rows:] + bdot(xh, low_ref[...], 1, 0)


def permuted_exact(x, one_hot):
    x1 = x.astype(bf16)
    rest = x - x1.astype(f32)
    x2 = rest.astype(bf16)
    x3 = (rest - x2.astype(f32)).astype(bf16)
    return bdot(x1, one_hot, 1, 1) + bdot(x2, one_hot, 1, 1) + bdot(x3, one_hot, 1, 1)


def prepare_kernel(
    schur, modes, count, order, later, load, coarse, rhs, scale,
    high, low, basis, to_right, to_left, payload,
):
    face = order.shape[1]
    k = modes.shape[0]
    cases = rhs.shape[0]
    nc = coarse.shape[1]
    hit = lax.broadcasted_iota(jnp.int32, (face, face), 0) == order[...]
    one_hot = jnp.where(hit, -1.0 * later[0].astype(f32), 0.0).astype(bf16)
    sh, sl = halves(schur[...])
    for part, out in ((sh, high), (sl, low)):
        top = bdot(one_hot, part[:face], 1, 0).astype(bf16)
        out[:face, :face] = bdot(top[:, :face], one_hot, 1, 1).astype(bf16)
        out[:face, face:] = top[:, face:]
        out[face:, :face] = bdot(part[face:, :face], one_hot, 1, 1).astype(bf16)
        out[face:, face:] = part[face:, face:]
    used = lax.broadcasted_iota(jnp.int32, (k, 1), 0) < count[0]
    masked = jnp.where(used, modes[...], 0.0)
    left = permuted_exact(masked[:, :face], one_hot)
    basis[...] = jnp.zeros_like(basis)
    basis[:k, :face] = left
    basis[:k, face:] = masked[:, face:]
    to_left[...] = jnp.zeros_like(to_left)
    to_left[:k] = left
    to_right[...] = jnp.zeros_like(to_right)
    to_right[:k] = masked[:, face:]
    to_right[PAD : PAD + cases] = rhs[...]
    to_right[PAD + cases : PAD + cases + 1] = scale[...]
    payload[...] = jnp.zeros_like(payload)
    peers = payload.shape[0]
    payload[:, :k, :nc] = jnp.broadcast_to(coarse[...][None], (peers, k, nc))
    payload[:, :k, nc : nc + cases] = jnp.broadcast_to(
        jnp.where(used, load[...], 0.0)[None], (peers, k, cases)
    )


def coarse_times(rows_ref, nc, values, packed, k):
    for i in range(nc // k):
        packed[i * k : (i + 1) * k] = values[i * PAD : i * PAD + k]
    return nn(rows_ref[:, :nc], packed[...])


def near_blocks(values, padded, here, stride):
    rows = values.shape[0]
    padded[:stride] = jnp.zeros((stride, values.shape[1]), f32)
    padded[stride + rows :] = jnp.zeros((stride, values.shape[1]), f32)
    padded[stride : stride + rows] = values
    start = here * PAD
    return jnp.concatenate(
        [padded[pl.ds(pl.multiple_of(start + b * stride, PAD), PAD), :] for b in range(3)], axis=0
    )


def gather_sum(wide, first, cases, stride):
    part = [wide[:, first + b * cases : first + (b + 1) * cases] for b in range(3)]
    none = jnp.zeros((stride, cases), f32)
    return (
        part[1]
        + jnp.concatenate([part[0][stride:], none], axis=0)
        + jnp.concatenate([none, part[2][:-stride]], axis=0)
    )


def scaled_gram_times(wide, first, values, k, near):
    rows, cases = values.shape
    blocks = rows // PAD
    matrix = wide[:, first : first + 3 * PAD].reshape(blocks, PAD, 3 * PAD)
    vector = values.reshape(blocks, PAD, cases)
    none = jnp.zeros((near, PAD, cases), f32)
    moved = [
        jnp.concatenate([none, vector[:-near]], axis=0),
        vector,
        jnp.concatenate([vector[near:], none], axis=0),
    ]
    total = jnp.zeros((blocks, PAD, cases), f32)
    for b in range(3):
        for m in range(k):
            total = total + matrix[:, :, b * PAD + m : b * PAD + m + 1] * moved[b][:, m : m + 1, :]
    return total.reshape(rows, cases)


def side_by_side(tall, blocks):
    return [tall[b * PAD : (b + 1) * PAD] for b in range(blocks)]


def start_kernel(
    here, gathered, high, low, basis, from_left, from_right, rhs, scale,
    frame, lifted_rhs, lifted_scale, start, v_left, v_right, payload, packed, padded, *, stride, k,
):
    face = rhs.shape[1]
    cases = rhs.shape[0]
    nc = packed.shape[0]
    y = coarse_times(gathered, nc, gathered[:, nc : nc + cases], packed, k)
    near = near_blocks(y, padded, here[0], stride)
    zero = jnp.zeros((PAD, face), f32)
    v = jnp.concatenate(
        [
            jnp.concatenate([from_left[:PAD], zero], axis=1),
            basis[...],
            jnp.concatenate([zero, from_right[...]], axis=1),
        ],
        axis=0,
    )
    frame[...] = v
    lb = jnp.concatenate([from_left[PAD : PAD + cases], rhs[...]], axis=1)
    ld = jnp.concatenate([from_left[PAD + cases : PAD + cases + 1], scale[...]], axis=1)
    lifted_rhs[...] = lb
    lifted_scale[...] = ld
    m0 = tn(near, v)
    start[...] = m0[:, face:]
    image = times_schur(m0, high, low)
    v_left[...] = image[:, :face]
    v_right[...] = image[:, face:]
    both = jnp.concatenate([v, v * ld], axis=0)
    shares = -nt(both, image)
    own = nt(jnp.concatenate([basis[...], basis[...] * ld], axis=0), lb)
    scaled = nt(basis[...] * ld, v)
    part = side_by_side(shares, 6)
    part[1] = part[1] + own[:PAD]
    part[4] = part[4] + own[PAD:]
    used = 6 * cases + 3 * PAD
    width = payload.shape[2]
    row = jnp.concatenate(part + [scaled, jnp.zeros((PAD, width - used), f32)], axis=1)
    payload[...] = jnp.broadcast_to(row[None], payload.shape)


def direction_kernel(
    here, gathered, coarse, high, low, frame, lifted_rhs, lifted_scale, m_left, m_right,
    from_left, from_right,
    search, residual, v_left, v_right, payload, packed, padded, *, stride, k,
):
    cases, face = m_left.shape
    nc = packed.shape[0]
    wide = gathered[...]
    g = gather_sum(wide, 0, cases, stride)
    h = gather_sum(wide, 3 * cases, cases, stride)
    c1 = coarse_times(coarse, nc, g, packed, k)
    c2 = coarse_times(
        coarse, nc, h - scaled_gram_times(wide, 6 * cases, c1, k, stride // PAD), packed, k
    )
    near1 = near_blocks(c1, padded, here[0], stride)
    near2 = near_blocks(c2, padded, here[0], stride)
    moved = jnp.concatenate([m_left[...] + from_left[...], m_right[...] + from_right[...]], axis=1)
    v = frame[...]
    r = lifted_rhs[...] - moved - tn(near1, v)
    s = lifted_scale[...] * r - tn(near2, v)
    search[...] = s
    residual[...] = r[:, face:]
    image = times_schur(s, high, low)
    v_left[...] = image[:, :face]
    v_right[...] = image[:, face:]
    shares = nt(jnp.concatenate([v, v * lifted_scale[...]], axis=0), image)
    energy = nt(s, image)
    part = side_by_side(shares, 6) + side_by_side(energy, cases // PAD)
    used = (6 + cases // PAD) * cases
    width = payload.shape[2]
    if width > used:
        part = part + [jnp.zeros((PAD, width - used), f32)]
    payload[...] = jnp.broadcast_to(jnp.concatenate(part, axis=1)[None], payload.shape)


def second_kernel(
    here, gathered, scaled, coarse, high, low, frame, lifted_scale, search, residual,
    s_left, s_right, from_left, from_right,
    projected, second, v_left, v_right, curvature, payload, packed, padded, *, stride, k,
):
    cases, face = s_left.shape
    nc = packed.shape[0]
    wide = gathered[...]
    g = gather_sum(wide, 0, cases, stride)
    h = gather_sum(wide, 3 * cases, cases, stride)
    for b in range(cases // PAD):
        piece = wide[:, (6 + b) * cases : (7 + b) * cases]
        curvature[b * PAD : (b + 1) * PAD] = piece.reshape(-1, PAD, cases).sum(axis=0)
    c1 = coarse_times(coarse, nc, g, packed, k)
    c2 = coarse_times(
        coarse, nc, h - scaled_gram_times(scaled[...], 6 * cases, c1, k, stride // PAD), packed, k
    )
    near1 = near_blocks(c1, padded, here[0], stride)
    near2 = near_blocks(c2, padded, here[0], stride)
    q = jnp.concatenate([s_left[...] + from_left[...], s_right[...] + from_right[...]], axis=1)
    v = frame[...]
    p = q - tn(near1, v)
    z = lifted_scale[...] * p - tn(near2, v)
    projected[...] = p[:, face:]
    zr = z[:, face:]
    second[...] = zr
    image = times_schur(z, high, low)
    v_left[...] = image[:, :face]
    v_right[...] = image[:, face:]
    r = residual[...]
    grams = nt(
        jnp.concatenate([search[:, face:], zr], axis=0),
        jnp.concatenate([r, p[:, face:], q[:, face:]], axis=0),
    )
    energy = nt(z, image)
    shares = side_by_side(nt(v, image), 3)
    top, bottom = grams[:cases], grams[cases:]
    crossed = nt(q[:, face:], zr)
    extra_top = jnp.concatenate(shares[:2], axis=1)
    extra_low = jnp.concatenate([shares[2], jnp.zeros((PAD, cases), f32)], axis=1)
    extra = jnp.concatenate([extra_top, extra_low], axis=0)
    row = [top[:, : 2 * cases], crossed, bottom[:, : 2 * cases], energy, extra]
    used = 8 * cases
    width = payload.shape[2]
    if width > used:
        row = row + [jnp.zeros((cases, width - used), f32)]
    payload[...] = jnp.broadcast_to(jnp.concatenate(row, axis=1)[None], payload.shape)


def eliminate(matrix, right):
    n = matrix.shape[0]
    work = jnp.concatenate([matrix, right], axis=1)
    rows = lax.broadcasted_iota(jnp.int32, work.shape, 0)
    for i in range(n):
        row = work[i : i + 1] / work[i : i + 1, i : i + 1]
        work = jnp.where(rows == i, row, work - work[:, i : i + 1] * row)
    return work[:, n:]


def finish_kernel(
    here, gathered, coarse, frame, start, search, residual, projected, second, curvature,
    v_right, from_right, out_mult, out_res, packed, *, stride, k, near,
):
    cases, face = start.shape
    nc = packed.shape[0]
    all_of = gathered[...]
    peers = all_of.shape[0]
    total = all_of.sum(axis=0)
    block = [total[:, b * cases : (b + 1) * cases] for b in range(6)]
    sr, sp, qz, zr, zp, zw = block
    low, mid = 6 * cases, 7 * cases
    part = [all_of[:, :PAD, low:mid], all_of[:, :PAD, mid : mid + cases], all_of[:, PAD : 2 * PAD, low:mid]]
    none = jnp.zeros((near, PAD, cases), f32)
    g = (
        part[1]
        + jnp.concatenate([part[0][near:], none], axis=0)
        + jnp.concatenate([none, part[2][:-near]], axis=0)
    ).reshape(peers * PAD, cases)
    for i in range(nc // k):
        packed[i * k : (i + 1) * k] = g[i * PAD : i * PAD + k]
    row = pl.multiple_of(here[0] * PAD, PAD)
    after = pl.multiple_of(here[1] * PAD, PAD)
    rows = jnp.concatenate([coarse[pl.ds(row, PAD), :nc], coarse[pl.ds(after, PAD), :nc]], axis=0)
    coefficients = nn(rows, packed[...])
    frame_right = frame[PAD : 3 * PAD, face:]
    w = v_right[...] + from_right[...] - tn(coefficients, frame_right)
    w0 = curvature[...]
    solved = eliminate(w0, jnp.concatenate([sr, qz], axis=1))
    a0, y = solved[:, :cases], solved[:, cases:]
    x = nn(y, a0)
    w1 = tn(a0, nn(zw, a0) - tn(qz, x))
    e1 = tn(x, sr - nn(sp, a0)) - tn(a0, zr - nn(zp, a0))
    a1 = eliminate(w1, e1)
    first = a0 + nn(x, a1)
    last = nn(a0, a1)
    out_mult[...] = start[...] + tn(first, search[:, face:]) - tn(last, second[...])
    out_res[...] = residual[...] - tn(first, projected[...]) + tn(last, w)


VMEM = pl.BlockSpec(memory_space=pltpu.VMEM)
SMEM = pl.BlockSpec(memory_space=pltpu.SMEM)


def call(kernel, args, outs, scratch, name, scalars):
    return pl.pallas_call(
        kernel,
        out_shape=[jax.ShapeDtypeStruct(s, d) for s, d in outs],
        in_specs=[SMEM if i in scalars else VMEM for i in range(len(args))],
        out_specs=[VMEM] * len(outs),
        scratch_shapes=[pltpu.VMEM(s, f32) for s in scratch],
        name=name,
    )(*args)


def exchange(to_right, to_left):
    n = lax.axis_size("cluster")
    from_left = lax.ppermute(to_right, "cluster", [(i, i + 1) for i in range(n - 1)])
    from_right = lax.ppermute(to_left, "cluster", [(i + 1, i) for i in range(n - 1)])
    return from_left, from_right


def spread(payload):
    return lax.all_to_all(payload, AXES, 0, 0)


def up(value, unit):
    return -(-value // unit) * unit


def shards(rhs, schur, modes, count, order, scale, load, coarse):
    chain = lax.axis_size("cluster")
    subs = lax.axis_size("sub")
    peers = chain * subs
    cases, face = rhs.shape[2:]
    size = schur.shape[2]
    k = modes.shape[2]
    nc = coarse.shape[1]
    stride = subs * PAD
    rows = peers * PAD
    at = lax.axis_index("cluster")
    me = at * subs + lax.axis_index("sub")
    here = jnp.stack([me, jnp.minimum(me + subs, peers - 1)]).astype(jnp.int32)
    later = (at > 0).astype(jnp.int32).reshape(1)
    rhs, schur, modes, load = rhs[0, 0], schur[0, 0], modes[0, 0], load[0, 0]
    count = count.reshape(1)
    order = order.reshape(1, face)
    scale = scale.reshape(1, face)
    vec = (cases, face)
    wide0 = up(nc + cases, 128)
    wide1 = up(6 * cases + 3 * PAD, 128)
    wide2 = up((6 + cases // PAD) * cases, 128)
    wide3 = up(8 * cases, 128)
    work = [(nc, cases), (rows + 2 * stride, cases)]
    head = functools.partial
    packet = up(PAD + cases + 1, 8)

    high, low, basis, to_right, to_left, payload = call(
        prepare_kernel,
        (schur, modes, count, order, later, load, coarse, rhs, scale),
        [
            ((size, size), bf16), ((size, size), bf16), ((PAD, size), f32),
            ((packet, face), f32), ((PAD, face), f32), ((peers, PAD, wide0), f32),
        ],
        [],
        "prepare",
        (2, 4),
    )
    from_left, from_right = exchange(to_right, to_left)
    coarse_rows = spread(payload).reshape(rows, wide0)

    frame, lifted_rhs, lifted_scale, start, m_left, m_right, payload = call(
        head(start_kernel, stride=stride, k=k),
        (here, coarse_rows, high, low, basis, from_left, from_right, rhs, scale),
        [
            ((3 * PAD, size), f32), ((cases, size), f32), ((1, size), f32), (vec, f32),
            (vec, f32), (vec, f32), ((peers, PAD, wide1), f32),
        ],
        work,
        "start",
        (0,),
    )
    from_left, from_right = exchange(m_right, m_left)
    first = spread(payload).reshape(rows, wide1)

    search, residual, s_left, s_right, payload = call(
        head(direction_kernel, stride=stride, k=k),
        (here, first, coarse_rows, high, low, frame, lifted_rhs, lifted_scale, m_left, m_right,
         from_left, from_right),
        [((cases, size), f32), (vec, f32), (vec, f32), (vec, f32), ((peers, PAD, wide2), f32)],
        work,
        "direction",
        (0,),
    )
    from_left, from_right = exchange(s_right, s_left)
    shared = spread(payload).reshape(rows, wide2)

    projected, second, z_left, z_right, curvature, payload = call(
        head(second_kernel, stride=stride, k=k),
        (here, shared, first, coarse_rows, high, low, frame, lifted_scale, search, residual,
         s_left, s_right, from_left, from_right),
        [(vec, f32), (vec, f32), (vec, f32), (vec, f32), ((cases, cases), f32),
         ((peers, cases, wide3), f32)],
        work,
        "second",
        (0,),
    )
    from_right = lax.ppermute(z_left, "cluster", [(i + 1, i) for i in range(chain - 1)])
    shared = spread(payload)

    multipliers, residual = call(
        head(finish_kernel, stride=stride, k=k, near=subs),
        (here, shared, coarse_rows, frame, start, search, residual, projected, second, curvature,
         z_right, from_right),
        [(vec, f32), (vec, f32)],
        [(nc, cases)],
        "finish",
        (0,),
    )
    return multipliers[None, None], residual[None, None]


def solution(mesh):
    in_specs = (
        P("sub", "cluster", None, None),
        P("sub", "cluster", None, None),
        P("sub", "cluster", None, None),
        P("sub", "cluster"),
        P("sub", "cluster", None),
        P("sub", "cluster", None),
        P("sub", "cluster", None, None),
        P(("cluster", "sub"), None),
    )
    out_specs = (P("sub", "cluster", None, None), P("sub", "cluster", None, None))
    return jax.shard_map(shards, mesh=mesh, in_specs=in_specs, out_specs=out_specs, check_vma=False)
```

```python
import functools
import math
import jax
import jax.numpy as jnp
from jax import lax
from jax.experimental import pallas as pl
from jax.experimental.pallas import tpu as pltpu
from jax.sharding import PartitionSpec as P

AXES = ("cluster", "sub")
f32 = jnp.float32
bf16 = jnp.bfloat16
PAD = 8


def dot(a, b, ca, cb):
    return lax.dot_general(
        a, b, (((ca,), (cb,)), ((), ())), precision=lax.Precision.HIGHEST, preferred_element_type=f32
    )


def nn(a, b):
    return dot(a, b, 1, 0)


def nt(a, b):
    return dot(a, b, 1, 1)


def tn(a, b):
    return dot(a, b, 0, 0)


def bdot(a, b, ca, cb):
    return lax.dot_general(a, b, (((ca,), (cb,)), ((), ())), preferred_element_type=f32)


def halves(x):
    high = x.astype(bf16)
    return high, (x - high.astype(f32)).astype(bf16)


def times_schur(x, high_ref, low_ref):
    rows = x.shape[0]
    xh, xl = halves(x)
    both = bdot(jnp.concatenate([xh, xl], axis=0), high_ref[...], 1, 0)
    return both[:rows] + both[rows:] + bdot(xh, low_ref[...], 1, 0)


def permuted_exact(x, one_hot):
    x1 = x.astype(bf16)
    rest = x - x1.astype(f32)
    x2 = rest.astype(bf16)
    x3 = (rest - x2.astype(f32)).astype(bf16)
    return bdot(x1, one_hot, 1, 1) + bdot(x2, one_hot, 1, 1) + bdot(x3, one_hot, 1, 1)


def split_sides(me, subs, right, left):
    even = (me // subs) % 2 == 0
    return jnp.where(even, right, left), jnp.where(even, left, right)


def join_sides(me, subs, chain, even_got, odd_got):
    at = me // subs
    even = at % 2 == 0
    left = jnp.where(even, odd_got, even_got)
    right = jnp.where(even, even_got, odd_got)
    return jnp.where(at > 0, left, 0.0), jnp.where(at < chain - 1, right, 0.0)


def signed_one_hot(me, subs, order):
    face = order.shape[1]
    hit = lax.broadcasted_iota(jnp.int32, (face, face), 0) == order
    sign = jnp.where(me // subs > 0, -1.0, 0.0)
    return jnp.where(hit, sign, 0.0).astype(bf16)


def pack_kernel(
    me, count, modes_in, order_in, load_in, coarse_in, rhs_in, scale_in,
    basis, own, to_even, to_odd, payload,
    modes, order, load, coarse, rhs, scale, sems, *, subs,
):
    pairs = (
        (order_in, order), (modes_in, modes), (coarse_in, coarse), (rhs_in, rhs),
        (scale_in, scale), (load_in, load),
    )
    copies = [pltpu.make_async_copy(a, b, sems.at[i]) for i, (a, b) in enumerate(pairs)]
    for copy in copies:
        copy.start()
    payload[...] = jnp.zeros_like(payload)
    own[...] = jnp.zeros_like(own)
    basis[...] = jnp.zeros_like(basis)
    face = order.shape[1]
    k = modes.shape[0]
    cases = rhs.shape[0]
    nc = coarse.shape[1]
    copies[0].wait()
    one_hot = signed_one_hot(me[0], subs, order[...])
    for copy in copies[1:]:
        copy.wait()
    used = lax.broadcasted_iota(jnp.int32, (k, 1), 0) < count[0]
    for i in range(k):
        basis[i : i + 1] = jnp.where(i < count[0], modes[i], 0.0)
    left = permuted_exact(basis[:, :face], one_hot)
    basis[:, :face] = left
    own[:PAD] = basis[:, face:]
    own[PAD : PAD + cases] = rhs[...]
    own[PAD + cases : PAD + cases + 1] = scale[...]
    rest = jnp.zeros((own.shape[0] - PAD, face), f32)
    to_even[...], to_odd[...] = split_sides(
        me[0], subs, own[...], jnp.concatenate([left, rest], axis=0)
    )
    peers = payload.shape[0]
    payload[:, :k, :nc] = jnp.broadcast_to(coarse[...][None], (peers, k, nc))
    for i in range(k):
        row = jnp.where(i < count[0], load[i], 0.0)
        payload[:, i : i + 1, nc : nc + cases] = jnp.broadcast_to(row[None], (peers, 1, cases))


def permute_kernel(me, order, schur, high, low, *, subs):
    face = order.shape[1]
    one_hot = signed_one_hot(me[0], subs, order[...])
    sh, sl = halves(schur[...])
    for part, out in ((sh, high), (sl, low)):
        top = bdot(one_hot, part[:face], 1, 0).astype(bf16)
        out[:face, :face] = bdot(top[:, :face], one_hot, 1, 1).astype(bf16)
        out[:face, face:] = top[:, face:]
        out[face:, :face] = bdot(part[face:, :face], one_hot, 1, 1).astype(bf16)
        out[face:, face:] = part[face:, face:]


def coarse_times(rows_ref, nc, values, packed, k):
    for i in range(nc // k):
        packed[i * k : (i + 1) * k] = values[i * PAD : i * PAD + k]
    return nn(rows_ref[:, :nc], packed[...])


def near_blocks(values, padded, here, stride):
    rows = values.shape[0]
    padded[:stride] = jnp.zeros((stride, values.shape[1]), f32)
    padded[stride + rows :] = jnp.zeros((stride, values.shape[1]), f32)
    padded[stride : stride + rows] = values
    start = here * PAD
    return jnp.concatenate(
        [padded[pl.ds(pl.multiple_of(start + b * stride, PAD), PAD), :] for b in range(3)], axis=0
    )


def gather_sum(wide, first, cases, stride):
    part = [wide[:, first + b * cases : first + (b + 1) * cases] for b in range(3)]
    none = jnp.zeros((stride, cases), f32)
    return (
        part[1]
        + jnp.concatenate([part[0][stride:], none], axis=0)
        + jnp.concatenate([none, part[2][:-stride]], axis=0)
    )


def scaled_gram_times(wide, first, values, k, near):
    rows, cases = values.shape
    blocks = rows // PAD
    matrix = wide[:, first : first + 3 * PAD].reshape(blocks, PAD, 3 * PAD)
    vector = values.reshape(blocks, PAD, cases)
    none = jnp.zeros((near, PAD, cases), f32)
    moved = [
        jnp.concatenate([none, vector[:-near]], axis=0),
        vector,
        jnp.concatenate([vector[near:], none], axis=0),
    ]
    total = jnp.zeros((blocks, PAD, cases), f32)
    for b in range(3):
        for m in range(k):
            total = total + matrix[:, :, b * PAD + m : b * PAD + m + 1] * moved[b][:, m : m + 1, :]
    return total.reshape(rows, cases)


def side_by_side(tall, blocks):
    return [tall[b * PAD : (b + 1) * PAD] for b in range(blocks)]


def load_kernel(me, gathered, near, packed, padded, *, stride, k):
    nc, cases = packed.shape
    y = coarse_times(gathered, nc, gathered[:, nc : nc + cases], packed, k)
    near[...] = near_blocks(y, padded, me[0], stride)


def start_kernel(
    me, near, high, low, basis, own, even_got, odd_got,
    frame, lifted_rhs, lifted_scale, start, image_out, to_even, to_odd, payload, *, subs, chain,
):
    face = own.shape[1]
    cases = near.shape[1]
    from_left, from_right = join_sides(me[0], subs, chain, even_got[...], odd_got[...])
    zero = jnp.zeros((PAD, face), f32)
    v = jnp.concatenate(
        [
            jnp.concatenate([from_left[:PAD], zero], axis=1),
            basis[...],
            jnp.concatenate([zero, from_right[:PAD]], axis=1),
        ],
        axis=0,
    )
    frame[...] = v
    both = jnp.concatenate([from_left, own[...]], axis=1)
    lb = both[PAD : PAD + cases]
    ld = both[PAD + cases : PAD + cases + 1]
    lifted_rhs[...] = lb
    lifted_scale[...] = ld
    m0 = tn(near[...], v)
    start[...] = m0[:, face:]
    image = times_schur(m0, high, low)
    image_out[...] = image
    to_even[...], to_odd[...] = split_sides(me[0], subs, image[:, face:], image[:, :face])
    shares = -nt(jnp.concatenate([v, v * ld], axis=0), image)
    mine = nt(jnp.concatenate([basis[...], basis[...] * ld], axis=0), lb)
    scaled = nt(basis[...] * ld, v)
    part = side_by_side(shares, 6)
    part[1] = part[1] + mine[:PAD]
    part[4] = part[4] + mine[PAD:]
    used = 6 * cases + 3 * PAD
    width = payload.shape[2]
    row = jnp.concatenate(part + [scaled, jnp.zeros((PAD, width - used), f32)], axis=1)
    payload[...] = jnp.broadcast_to(row[None], payload.shape)


def project_kernel(me, gathered, scaled, coarse, near, curvature, packed, padded, *, stride, k):
    nc, cases = packed.shape
    wide = gathered[...]
    g = gather_sum(wide, 0, cases, stride)
    h = gather_sum(wide, 3 * cases, cases, stride)
    c1 = coarse_times(coarse, nc, g, packed, k)
    c2 = coarse_times(
        coarse, nc, h - scaled_gram_times(scaled[...], 6 * cases, c1, k, stride // PAD), packed, k
    )
    near[: 3 * PAD] = near_blocks(c1, padded, me[0], stride)
    near[3 * PAD :] = near_blocks(c2, padded, me[0], stride)
    for b in range(cases // PAD):
        piece = wide[:, (6 + b) * cases : (7 + b) * cases]
        curvature[b * PAD : (b + 1) * PAD] = piece.reshape(-1, PAD, cases).sum(axis=0)


def direction_kernel(
    me, near, high, low, frame, lifted_rhs, lifted_scale, image_in, even_got, odd_got,
    search, residual, image_out, to_even, to_odd, payload, *, subs, chain,
):
    cases, face = even_got.shape
    from_left, from_right = join_sides(me[0], subs, chain, even_got[...], odd_got[...])
    moved = image_in[...] + jnp.concatenate([from_left, from_right], axis=1)
    v = frame[...]
    r = lifted_rhs[...] - moved - tn(near[: 3 * PAD], v)
    s = lifted_scale[...] * r - tn(near[3 * PAD :], v)
    search[...] = s
    residual[...] = r[:, face:]
    image = times_schur(s, high, low)
    image_out[...] = image
    to_even[...], to_odd[...] = split_sides(me[0], subs, image[:, face:], image[:, :face])
    shares = nt(jnp.concatenate([v, v * lifted_scale[...]], axis=0), image)
    energy = nt(s, image)
    part = side_by_side(shares, 6) + side_by_side(energy, cases // PAD)
    used = (6 + cases // PAD) * cases
    width = payload.shape[2]
    if width > used:
        part = part + [jnp.zeros((PAD, width - used), f32)]
    payload[...] = jnp.broadcast_to(jnp.concatenate(part, axis=1)[None], payload.shape)


def second_kernel(
    me, near, high, low, frame, lifted_scale, search, residual, image_in, even_got, odd_got,
    projected, second, image_out, to_even, to_odd, payload, *, subs, chain,
):
    cases, face = even_got.shape
    from_left, from_right = join_sides(me[0], subs, chain, even_got[...], odd_got[...])
    q = image_in[...] + jnp.concatenate([from_left, from_right], axis=1)
    v = frame[...]
    p = q - tn(near[: 3 * PAD], v)
    z = lifted_scale[...] * p - tn(near[3 * PAD :], v)
    projected[...] = p[:, face:]
    zr = z[:, face:]
    second[...] = zr
    image = times_schur(z, high, low)
    image_out[...] = image[:, face:]
    to_even[...], to_odd[...] = split_sides(me[0], subs, image[:, face:], image[:, :face])
    grams = nt(
        jnp.concatenate([search[:, face:], zr, q[:, face:]], axis=0),
        jnp.concatenate([residual[...], p[:, face:], zr], axis=0),
    )
    energy = nt(z, image)
    shares = side_by_side(nt(v, image), 3)
    top, bottom = grams[:cases, : 2 * cases], grams[cases : 2 * cases, : 2 * cases]
    crossed = grams[2 * cases :, 2 * cases :]
    extra_top = jnp.concatenate(shares[:2], axis=1)
    extra_low = jnp.concatenate([shares[2], jnp.zeros((PAD, cases), f32)], axis=1)
    extra = jnp.concatenate([extra_top, extra_low], axis=0)
    row = [top, crossed, bottom, energy, extra]
    used = 8 * cases
    width = payload.shape[2]
    if width > used:
        row = row + [jnp.zeros((cases, width - used), f32)]
    payload[...] = jnp.broadcast_to(jnp.concatenate(row, axis=1)[None], payload.shape)


def eliminate(matrix, right):
    n = matrix.shape[0]
    work = jnp.concatenate([matrix, right], axis=1)
    rows = lax.broadcasted_iota(jnp.int32, work.shape, 0)
    for i in range(n):
        row = work[i : i + 1] / work[i : i + 1, i : i + 1]
        work = jnp.where(rows == i, row, work - work[:, i : i + 1] * row)
    return work[:, n:]


def invert_kernel(curvature, inverse):
    n = curvature.shape[0]
    rows = lax.broadcasted_iota(jnp.int32, (n, n), 0)
    columns = lax.broadcasted_iota(jnp.int32, (n, n), 1)
    inverse[...] = eliminate(curvature[...], jnp.where(rows == columns, 1.0, 0.0))


def step_kernel(me, gathered, coarse, inverse, steps, packed, *, subs, chain, k):
    nc, cases = packed.shape
    all_of = gathered[...]
    peers = all_of.shape[0]
    total = all_of.sum(axis=0)
    sr, sp, qz, zr, zp, zw = [total[:, b * cases : (b + 1) * cases] for b in range(6)]
    low, mid = 6 * cases, 7 * cases
    part = [
        all_of[:, :PAD, low:mid],
        all_of[:, :PAD, mid : mid + cases],
        all_of[:, PAD : 2 * PAD, low:mid],
    ]
    none = jnp.zeros((subs, PAD, cases), f32)
    g = (
        part[1]
        + jnp.concatenate([part[0][subs:], none], axis=0)
        + jnp.concatenate([none, part[2][:-subs]], axis=0)
    ).reshape(peers * PAD, cases)
    for i in range(nc // k):
        packed[i * k : (i + 1) * k] = g[i * PAD : i * PAD + k]
    row = pl.multiple_of(me[0] * PAD, PAD)
    after = pl.multiple_of(jnp.minimum(me[0] + subs, peers - 1) * PAD, PAD)
    rows = jnp.concatenate([coarse[pl.ds(row, PAD), :nc], coarse[pl.ds(after, PAD), :nc]], axis=0)
    own = nn(rows, packed[...])
    solved = nn(inverse[...], jnp.concatenate([sr, qz], axis=1))
    a0, y = solved[:, :cases], solved[:, cases:]
    x = nn(y, a0)
    w1 = tn(a0, nn(zw, a0) - tn(qz, x))
    e1 = tn(x, sr - nn(sp, a0)) - tn(a0, zr - nn(zp, a0))
    a1 = eliminate(w1, e1)
    steps[:cases] = a0 + nn(x, a1)
    steps[cases : 2 * cases] = nn(a0, a1)
    steps[2 * cases :] = own


def finish_kernel(
    me, steps, frame, start, search, residual, projected, second, image, even_got, odd_got,
    out_mult, out_res, *, subs, chain,
):
    cases, face = start.shape
    _, from_right = join_sides(me[0], subs, chain, even_got[...], odd_got[...])
    w = image[...] + from_right - tn(steps[2 * cases :], frame[PAD : 3 * PAD, face:])
    first, last = steps[:cases], steps[cases : 2 * cases]
    out_mult[...] = start[...] + tn(first, search[:, face:]) - tn(last, second[...])
    out_res[...] = residual[...] - tn(first, projected[...]) + tn(last, w)


VMEM = pl.BlockSpec(memory_space=pltpu.VMEM)
SMEM = pl.BlockSpec(memory_space=pltpu.SMEM)
FAR = pl.BlockSpec(memory_space=pltpu.HBM)


def up(value, unit):
    return -(-value // unit) * unit


def call(kernel, args, outs, name, scratch=(), scalars=(0,), far=(), sems=0):
    shapes = [(a.shape, a.dtype) for i, a in enumerate(args) if i not in far + scalars]
    shapes = shapes + list(outs) + [(s, f32) for s in scratch if isinstance(s, tuple)]
    need = sum(math.prod(s[:-1]) * up(s[-1], 128) * jnp.dtype(d).itemsize for s, d in shapes)
    limit = 60 * 1024 * 1024 if far else min(2 * need + (6 << 20), 60 << 20)
    spaces = [SMEM if i in scalars else FAR if i in far else VMEM for i in range(len(args))]
    extra = [pltpu.SemaphoreType.DMA((sems,))] if sems else []
    return pl.pallas_call(
        kernel,
        out_shape=[jax.ShapeDtypeStruct(s, d) for s, d in outs],
        in_specs=spaces,
        out_specs=[VMEM] * len(outs),
        scratch_shapes=[s if not isinstance(s, tuple) else pltpu.VMEM(s, f32) for s in scratch] + extra,
        name=name,
        compiler_params=pltpu.CompilerParams(vmem_limit_bytes=limit),
    )(*args)


def exchange(to_even, to_odd):
    chain = lax.axis_size("cluster")
    subs = lax.axis_size("sub")
    even, odd = [], []
    for c in range(chain):
        for t in range(subs):
            even.append((c * subs + t, (c ^ 1) * subs + t))
            if c in (0, chain - 1):
                odd.append((c * subs + t, c * subs + (t ^ 1)))
            else:
                odd.append((c * subs + t, (((c + 1) ^ 1) - 1) * subs + t))
    return lax.ppermute(to_even, AXES, even), lax.ppermute(to_odd, AXES, odd)


def spread(payload):
    return lax.all_to_all(payload, AXES, 0, 0)


def shards(rhs, schur, modes, count, order, scale, load, coarse):
    chain = lax.axis_size("cluster")
    subs = lax.axis_size("sub")
    peers = chain * subs
    cases, face = rhs.shape[2:]
    size = schur.shape[2]
    k = modes.shape[2]
    nc = coarse.shape[1]
    stride = subs * PAD
    rows = peers * PAD
    me = (lax.axis_index("cluster") * subs + lax.axis_index("sub")).astype(jnp.int32).reshape(1)
    rhs, schur = rhs[0, 0], schur[0, 0]
    modes = modes[0].transpose(1, 0, 2)
    load = load[0].transpose(1, 0, 2)
    count = count.reshape(1)
    order = order.reshape(1, face)
    scale = scale.reshape(1, face)
    vec, lifted, small = (cases, face), (cases, size), (cases, cases)
    wide0 = up(nc + cases, 128)
    wide1 = up(6 * cases + 3 * PAD, 128)
    wide2 = up((6 + cases // PAD) * cases, 128)
    wide3 = up(8 * cases, 128)
    work = [(nc, cases), (rows + 2 * stride, cases)]
    packet = (up(PAD + cases + 1, 8), face)
    head = functools.partial
    line = {"subs": subs, "chain": chain}
    grid = {"stride": stride, "k": k}

    basis, own, to_even, to_odd, payload = call(
        head(pack_kernel, subs=subs),
        (me, count, modes, order, load, coarse, rhs, scale),
        [((PAD, size), f32), (packet, f32), (packet, f32), (packet, f32), ((peers, PAD, wide0), f32)],
        "pack",
        scratch=[modes.shape, pltpu.VMEM(order.shape, jnp.int32), load.shape, coarse.shape, vec, scale.shape],
        scalars=(0, 1),
        far=(2, 3, 4, 5, 6, 7),
        sems=6,
    )
    got = exchange(to_even, to_odd)
    coarse_rows = spread(payload).reshape(rows, wide0)
    high, low = call(
        head(permute_kernel, subs=subs),
        (me, order, schur),
        [((size, size), bf16), ((size, size), bf16)],
        "permute",
    )
    (near,) = call(
        head(load_kernel, **grid), (me, coarse_rows), [((3 * PAD, cases), f32)], "load", scratch=work
    )

    frame, lifted_rhs, lifted_scale, start, image, to_even, to_odd, payload = call(
        head(start_kernel, **line),
        (me, near, high, low, basis, own, *got),
        [
            ((3 * PAD, size), f32), (lifted, f32), ((1, size), f32), (vec, f32), (lifted, f32),
            (vec, f32), (vec, f32), ((peers, PAD, wide1), f32),
        ],
        "start",
    )
    got = exchange(to_even, to_odd)
    first = spread(payload).reshape(rows, wide1)
    near, _ = call(
        head(project_kernel, **grid),
        (me, first, first, coarse_rows),
        [((6 * PAD, cases), f32), (small, f32)],
        "project_start",
        scratch=work,
    )

    search, residual, image, to_even, to_odd, payload = call(
        head(direction_kernel, **line),
        (me, near, high, low, frame, lifted_rhs, lifted_scale, image, *got),
        [(lifted, f32), (vec, f32), (lifted, f32), (vec, f32), (vec, f32), ((peers, PAD, wide2), f32)],
        "direction",
    )
    got = exchange(to_even, to_odd)
    shared = spread(payload).reshape(rows, wide2)
    near, curvature = call(
        head(project_kernel, **grid),
        (me, shared, first, coarse_rows),
        [((6 * PAD, cases), f32), (small, f32)],
        "project_image",
        scratch=work,
    )

    projected, second, image, to_even, to_odd, payload = call(
        head(second_kernel, **line),
        (me, near, high, low, frame, lifted_scale, search, residual, image, *got),
        [(vec, f32), (vec, f32), (vec, f32), (vec, f32), (vec, f32), ((peers, cases, wide3), f32)],
        "second",
    )
    got = exchange(to_even, to_odd)
    shared = spread(payload)
    (inverse,) = call(invert_kernel, (curvature,), [(small, f32)], "invert", scalars=())
    (steps,) = call(
        head(step_kernel, k=k, **line),
        (me, shared, coarse_rows, inverse),
        [((2 * cases + 2 * PAD, cases), f32)],
        "step",
        scratch=[(nc, cases)],
    )
    multipliers, residual = call(
        head(finish_kernel, **line),
        (me, steps, frame, start, search, residual, projected, second, image, *got),
        [(vec, f32), (vec, f32)],
        "finish",
    )
    return multipliers[None, None], residual[None, None]


def solution(mesh):
    in_specs = (
        P("sub", "cluster", None, None),
        P("sub", "cluster", None, None),
        P("sub", "cluster", None, None),
        P("sub", "cluster"),
        P("sub", "cluster", None),
        P("sub", "cluster", None),
        P("sub", "cluster", None, None),
        P(("cluster", "sub"), None),
    )
    out_specs = (P("sub", "cluster", None, None), P("sub", "cluster", None, None))
    return jax.shard_map(shards, mesh=mesh, in_specs=in_specs, out_specs=out_specs, check_vma=False)
```

```python
import functools
import math
import jax
import jax.numpy as jnp
from jax import lax
from jax.experimental import pallas as pl
from jax.experimental.pallas import tpu as pltpu
from jax.sharding import PartitionSpec as P

AXES = ("cluster", "sub")
f32 = jnp.float32
bf16 = jnp.bfloat16
PAD = 8


def dot(a, b, ca, cb):
    return lax.dot_general(
        a, b, (((ca,), (cb,)), ((), ())), precision=lax.Precision.HIGHEST, preferred_element_type=f32
    )


def nn(a, b):
    return dot(a, b, 1, 0)


def nt(a, b):
    return dot(a, b, 1, 1)


def tn(a, b):
    return dot(a, b, 0, 0)


def bdot(a, b, ca, cb):
    return lax.dot_general(a, b, (((ca,), (cb,)), ((), ())), preferred_element_type=f32)


def halves(x):
    high = x.astype(bf16)
    return high, (x - high.astype(f32)).astype(bf16)


def times_schur(x, high_ref, low_ref):
    rows = x.shape[0]
    xh, xl = halves(x)
    both = bdot(jnp.concatenate([xh, xl], axis=0), high_ref[...], 1, 0)
    return both[:rows] + both[rows:] + bdot(xh, low_ref[...], 1, 0)


def permuted_exact(x, one_hot):
    x1 = x.astype(bf16)
    rest = x - x1.astype(f32)
    x2 = rest.astype(bf16)
    x3 = (rest - x2.astype(f32)).astype(bf16)
    return bdot(x1, one_hot, 1, 1) + bdot(x2, one_hot, 1, 1) + bdot(x3, one_hot, 1, 1)


def split_sides(me, subs, right, left):
    even = (me // subs) % 2 == 0
    return jnp.where(even, right, left), jnp.where(even, left, right)


def join_sides(me, subs, chain, even_got, odd_got):
    at = me // subs
    even = at % 2 == 0
    left = jnp.where(even, odd_got, even_got)
    right = jnp.where(even, even_got, odd_got)
    return jnp.where(at > 0, left, 0.0), jnp.where(at < chain - 1, right, 0.0)


def signed_one_hot(me, subs, order):
    face = order.shape[1]
    hit = lax.broadcasted_iota(jnp.int32, (face, face), 0) == order
    sign = jnp.where(me // subs > 0, -1.0, 0.0)
    return jnp.where(hit, sign, 0.0).astype(bf16)


def pack_kernel(
    me, count, modes_in, order_in, load_in, coarse_in, rhs_in, scale_in,
    basis, own, to_even, to_odd, payload,
    modes, order, load, coarse, rhs, scale, sems, *, subs,
):
    pairs = (
        (order_in, order), (modes_in, modes), (coarse_in, coarse), (rhs_in, rhs),
        (scale_in, scale), (load_in, load),
    )
    copies = [pltpu.make_async_copy(a, b, sems.at[i]) for i, (a, b) in enumerate(pairs)]
    for copy in copies:
        copy.start()
    own[...] = jnp.zeros_like(own)
    basis[...] = jnp.zeros_like(basis)
    face = order.shape[1]
    k = modes.shape[0]
    cases = rhs.shape[0]
    nc = coarse.shape[1]
    copies[0].wait()
    one_hot = signed_one_hot(me[0], subs, order[...])
    for copy in copies[1:]:
        copy.wait()
    used = lax.broadcasted_iota(jnp.int32, (k, 1), 0) < count[0]
    for i in range(k):
        basis[i : i + 1] = jnp.where(i < count[0], modes[i], 0.0)
    left = permuted_exact(basis[:, :face], one_hot)
    basis[:, :face] = left
    own[:PAD] = basis[:, face:]
    own[PAD : PAD + cases] = rhs[...]
    own[PAD + cases : PAD + cases + 1] = scale[...]
    rest = jnp.zeros((own.shape[0] - PAD, face), f32)
    to_even[...], to_odd[...] = split_sides(
        me[0], subs, own[...], jnp.concatenate([left, rest], axis=0)
    )
    peers = payload.shape[0]
    each = nc + cases
    line = []
    for i in range(k):
        line = line + [coarse[i : i + 1], jnp.where(i < count[0], load[i], 0.0)]
    line = line + [jnp.zeros((1, payload.shape[2] - k * each), f32)]
    payload[...] = jnp.broadcast_to(jnp.concatenate(line, axis=1)[None], payload.shape)


def permute_kernel(me, order, schur, high, low, *, subs):
    face = order.shape[1]
    one_hot = signed_one_hot(me[0], subs, order[...])
    sh, sl = halves(schur[...])
    for part, out in ((sh, high), (sl, low)):
        top = bdot(one_hot, part[:face], 1, 0).astype(bf16)
        out[:face, :face] = bdot(top[:, :face], one_hot, 1, 1).astype(bf16)
        out[:face, face:] = top[:, face:]
        out[face:, :face] = bdot(part[face:, :face], one_hot, 1, 1).astype(bf16)
        out[face:, face:] = part[face:, face:]


def coarse_times(rows_ref, nc, values, packed, k):
    for i in range(nc // k):
        packed[i * k : (i + 1) * k] = values[i * PAD : i * PAD + k]
    return nn(rows_ref[:, :nc], packed[...])


def near_blocks(values, padded, here, stride):
    rows = values.shape[0]
    padded[:stride] = jnp.zeros((stride, values.shape[1]), f32)
    padded[stride + rows :] = jnp.zeros((stride, values.shape[1]), f32)
    padded[stride : stride + rows] = values
    start = here * PAD
    return jnp.concatenate(
        [padded[pl.ds(pl.multiple_of(start + b * stride, PAD), PAD), :] for b in range(3)], axis=0
    )


def gather_sum(wide, first, cases, stride):
    part = [wide[:, first + b * cases : first + (b + 1) * cases] for b in range(3)]
    none = jnp.zeros((stride, cases), f32)
    return (
        part[1]
        + jnp.concatenate([part[0][stride:], none], axis=0)
        + jnp.concatenate([none, part[2][:-stride]], axis=0)
    )


def scaled_gram_times(wide, first, values, k, near):
    rows, cases = values.shape
    blocks = rows // PAD
    matrix = wide[:, first : first + 3 * PAD].reshape(blocks, PAD, 3 * PAD)
    vector = values.reshape(blocks, PAD, cases)
    none = jnp.zeros((near, PAD, cases), f32)
    moved = [
        jnp.concatenate([none, vector[:-near]], axis=0),
        vector,
        jnp.concatenate([vector[near:], none], axis=0),
    ]
    total = jnp.zeros((blocks, PAD, cases), f32)
    for b in range(3):
        for m in range(k):
            total = total + matrix[:, :, b * PAD + m : b * PAD + m + 1] * moved[b][:, m : m + 1, :]
    return total.reshape(rows, cases)


def side_by_side(tall, blocks):
    return [tall[b * PAD : (b + 1) * PAD] for b in range(blocks)]


def load_kernel(me, gathered, near, rows, packed, padded, *, stride, k):
    nc, cases = packed.shape
    each = nc + cases
    peers = gathered.shape[0]
    rows[...] = jnp.zeros_like(rows)
    for i in range(k):
        rows[:, i, :each] = gathered[:, 0, i * each : (i + 1) * each]
    for i in range(peers):
        packed[i * k : (i + 1) * k] = rows[i, :k, nc:each]
    table = rows[:, :, :nc].reshape(peers * PAD, nc)
    near[...] = near_blocks(nn(table, packed[...]), padded, me[0], stride)


def start_kernel(
    me, near, high, low, basis, own, even_got, odd_got,
    frame, lifted_rhs, lifted_scale, start, image_out, to_even, to_odd, payload, *, subs, chain,
):
    face = own.shape[1]
    cases = near.shape[1]
    from_left, from_right = join_sides(me[0], subs, chain, even_got[...], odd_got[...])
    zero = jnp.zeros((PAD, face), f32)
    v = jnp.concatenate(
        [
            jnp.concatenate([from_left[:PAD], zero], axis=1),
            basis[...],
            jnp.concatenate([zero, from_right[:PAD]], axis=1),
        ],
        axis=0,
    )
    frame[...] = v
    both = jnp.concatenate([from_left, own[...]], axis=1)
    lb = both[PAD : PAD + cases]
    ld = both[PAD + cases : PAD + cases + 1]
    lifted_rhs[...] = lb
    lifted_scale[...] = ld
    m0 = tn(near[...], v)
    start[...] = m0[:, face:]
    image = times_schur(m0, high, low)
    image_out[...] = image
    to_even[...], to_odd[...] = split_sides(me[0], subs, image[:, face:], image[:, :face])
    shares = -nt(jnp.concatenate([v, v * ld], axis=0), image)
    mine = nt(jnp.concatenate([basis[...], basis[...] * ld], axis=0), lb)
    scaled = nt(basis[...] * ld, v)
    part = side_by_side(shares, 6)
    part[1] = part[1] + mine[:PAD]
    part[4] = part[4] + mine[PAD:]
    used = 6 * cases + 3 * PAD
    width = payload.shape[2]
    row = jnp.concatenate(part + [scaled, jnp.zeros((PAD, width - used), f32)], axis=1)
    payload[...] = jnp.broadcast_to(row[None], payload.shape)


def project_kernel(me, gathered, scaled, coarse, near, curvature, packed, padded, *, stride, k, total):
    nc, cases = packed.shape
    wide = gathered[...]
    g = gather_sum(wide, 0, cases, stride)
    h = gather_sum(wide, 3 * cases, cases, stride)
    c1 = coarse_times(coarse, nc, g, packed, k)
    c2 = coarse_times(
        coarse, nc, h - scaled_gram_times(scaled[...], 6 * cases, c1, k, stride // PAD), packed, k
    )
    near[: 3 * PAD] = near_blocks(c1, padded, me[0], stride)
    near[3 * PAD :] = near_blocks(c2, padded, me[0], stride)
    if not total:
        curvature[...] = jnp.zeros_like(curvature)
    for b in range(cases // PAD if total else 0):
        piece = wide[:, (6 + b) * cases : (7 + b) * cases]
        curvature[b * PAD : (b + 1) * PAD] = piece.reshape(-1, PAD, cases).sum(axis=0)


def direction_kernel(
    me, near, high, low, frame, lifted_rhs, lifted_scale, image_in, even_got, odd_got,
    search, residual, image_out, to_even, to_odd, payload, *, subs, chain,
):
    cases, face = even_got.shape
    from_left, from_right = join_sides(me[0], subs, chain, even_got[...], odd_got[...])
    moved = image_in[...] + jnp.concatenate([from_left, from_right], axis=1)
    v = frame[...]
    r = lifted_rhs[...] - moved - tn(near[: 3 * PAD], v)
    s = lifted_scale[...] * r - tn(near[3 * PAD :], v)
    search[...] = s
    residual[...] = r[:, face:]
    image = times_schur(s, high, low)
    image_out[...] = image
    to_even[...], to_odd[...] = split_sides(me[0], subs, image[:, face:], image[:, :face])
    shares = nt(jnp.concatenate([v, v * lifted_scale[...]], axis=0), image)
    energy = nt(s, image)
    part = side_by_side(shares, 6) + side_by_side(energy, cases // PAD)
    used = (6 + cases // PAD) * cases
    width = payload.shape[2]
    if width > used:
        part = part + [jnp.zeros((PAD, width - used), f32)]
    payload[...] = jnp.broadcast_to(jnp.concatenate(part, axis=1)[None], payload.shape)


def second_kernel(
    me, near, high, low, frame, lifted_scale, search, residual, image_in, even_got, odd_got,
    projected, second, image_out, to_even, to_odd, payload, *, subs, chain,
):
    cases, face = even_got.shape
    from_left, from_right = join_sides(me[0], subs, chain, even_got[...], odd_got[...])
    q = image_in[...] + jnp.concatenate([from_left, from_right], axis=1)
    v = frame[...]
    p = q - tn(near[: 3 * PAD], v)
    z = lifted_scale[...] * p - tn(near[3 * PAD :], v)
    projected[...] = p[:, face:]
    zr = z[:, face:]
    second[...] = zr
    image = times_schur(z, high, low)
    image_out[...] = image[:, face:]
    to_even[...], to_odd[...] = split_sides(me[0], subs, image[:, face:], image[:, :face])
    grams = nt(
        jnp.concatenate([search[:, face:], zr, q[:, face:]], axis=0),
        jnp.concatenate([residual[...], p[:, face:], zr], axis=0),
    )
    energy = nt(z, image)
    shares = side_by_side(nt(v, image), 3)
    top, bottom = grams[:cases, : 2 * cases], grams[cases : 2 * cases, : 2 * cases]
    crossed = grams[2 * cases :, 2 * cases :]
    extra_top = jnp.concatenate(shares[:2], axis=1)
    extra_low = jnp.concatenate([shares[2], jnp.zeros((PAD, cases), f32)], axis=1)
    extra = jnp.concatenate([extra_top, extra_low], axis=0)
    row = [top, crossed, bottom, energy, extra]
    used = 8 * cases
    width = payload.shape[2]
    if width > used:
        row = row + [jnp.zeros((cases, width - used), f32)]
    payload[...] = jnp.broadcast_to(jnp.concatenate(row, axis=1)[None], payload.shape)


def eliminate(matrix, right):
    n = matrix.shape[0]
    work = jnp.concatenate([matrix, right], axis=1)
    rows = lax.broadcasted_iota(jnp.int32, work.shape, 0)
    for i in range(n):
        row = work[i : i + 1] / work[i : i + 1, i : i + 1]
        work = jnp.where(rows == i, row, work - work[:, i : i + 1] * row)
    return work[:, n:]


def invert_kernel(curvature, inverse):
    n = curvature.shape[0]
    rows = lax.broadcasted_iota(jnp.int32, (n, n), 0)
    columns = lax.broadcasted_iota(jnp.int32, (n, n), 1)
    inverse[...] = eliminate(curvature[...], jnp.where(rows == columns, 1.0, 0.0))


def step_kernel(me, gathered, coarse, inverse, steps, packed, *, subs, chain, k):
    nc, cases = packed.shape
    all_of = gathered[...]
    peers = all_of.shape[0]
    total = all_of.sum(axis=0)
    sr, sp, qz, zr, zp, zw = [total[:, b * cases : (b + 1) * cases] for b in range(6)]
    low, mid = 6 * cases, 7 * cases
    part = [
        all_of[:, :PAD, low:mid],
        all_of[:, :PAD, mid : mid + cases],
        all_of[:, PAD : 2 * PAD, low:mid],
    ]
    none = jnp.zeros((subs, PAD, cases), f32)
    g = (
        part[1]
        + jnp.concatenate([part[0][subs:], none], axis=0)
        + jnp.concatenate([none, part[2][:-subs]], axis=0)
    ).reshape(peers * PAD, cases)
    for i in range(nc // k):
        packed[i * k : (i + 1) * k] = g[i * PAD : i * PAD + k]
    row = pl.multiple_of(me[0] * PAD, PAD)
    after = pl.multiple_of(jnp.minimum(me[0] + subs, peers - 1) * PAD, PAD)
    rows = jnp.concatenate([coarse[pl.ds(row, PAD), :nc], coarse[pl.ds(after, PAD), :nc]], axis=0)
    own = nn(rows, packed[...])
    solved = nn(inverse[...], jnp.concatenate([sr, qz], axis=1))
    a0, y = solved[:, :cases], solved[:, cases:]
    x = nn(y, a0)
    w1 = tn(a0, nn(zw, a0) - tn(qz, x))
    e1 = tn(x, sr - nn(sp, a0)) - tn(a0, zr - nn(zp, a0))
    a1 = eliminate(w1, e1)
    steps[:cases] = a0 + nn(x, a1)
    steps[cases : 2 * cases] = nn(a0, a1)
    steps[2 * cases :] = own


def finish_kernel(
    me, steps, frame, start, search, residual, projected, second, image, even_got, odd_got,
    out_mult, out_res, *, subs, chain,
):
    cases, face = start.shape
    _, from_right = join_sides(me[0], subs, chain, even_got[...], odd_got[...])
    w = image[...] + from_right - tn(steps[2 * cases :], frame[PAD : 3 * PAD, face:])
    first, last = steps[:cases], steps[cases : 2 * cases]
    out_mult[...] = start[...] + tn(first, search[:, face:]) - tn(last, second[...])
    out_res[...] = residual[...] - tn(first, projected[...]) + tn(last, w)


VMEM = pl.BlockSpec(memory_space=pltpu.VMEM)
SMEM = pl.BlockSpec(memory_space=pltpu.SMEM)
FAR = pl.BlockSpec(memory_space=pltpu.HBM)


def up(value, unit):
    return -(-value // unit) * unit


def call(kernel, args, outs, name, scratch=(), scalars=(0,), far=(), sems=0):
    shapes = [(a.shape, a.dtype) for i, a in enumerate(args) if i not in far + scalars]
    shapes = shapes + list(outs) + [(s, f32) for s in scratch if isinstance(s, tuple)]
    need = sum(math.prod(s[:-1]) * up(s[-1], 128) * jnp.dtype(d).itemsize for s, d in shapes)
    limit = 60 * 1024 * 1024 if far else min(2 * need + (6 << 20), 60 << 20)
    spaces = [SMEM if i in scalars else FAR if i in far else VMEM for i in range(len(args))]
    extra = [pltpu.SemaphoreType.DMA((sems,))] if sems else []
    return pl.pallas_call(
        kernel,
        out_shape=[jax.ShapeDtypeStruct(s, d) for s, d in outs],
        in_specs=spaces,
        out_specs=[VMEM] * len(outs),
        scratch_shapes=[s if not isinstance(s, tuple) else pltpu.VMEM(s, f32) for s in scratch] + extra,
        name=name,
        compiler_params=pltpu.CompilerParams(vmem_limit_bytes=limit),
    )(*args)


def exchange(to_even, to_odd):
    chain = lax.axis_size("cluster")
    subs = lax.axis_size("sub")
    even, odd = [], []
    for c in range(chain):
        for t in range(subs):
            even.append((c * subs + t, (c ^ 1) * subs + t))
            if c in (0, chain - 1):
                odd.append((c * subs + t, c * subs + (t ^ 1)))
            else:
                odd.append((c * subs + t, (((c + 1) ^ 1) - 1) * subs + t))
    return lax.ppermute(to_even, AXES, even), lax.ppermute(to_odd, AXES, odd)


def spread(payload):
    return lax.all_to_all(payload, AXES, 0, 0)


def shards(rhs, schur, modes, count, order, scale, load, coarse):
    chain = lax.axis_size("cluster")
    subs = lax.axis_size("sub")
    peers = chain * subs
    cases, face = rhs.shape[2:]
    size = schur.shape[2]
    k = modes.shape[2]
    nc = coarse.shape[1]
    stride = subs * PAD
    rows = peers * PAD
    me = (lax.axis_index("cluster") * subs + lax.axis_index("sub")).astype(jnp.int32).reshape(1)
    rhs, schur = rhs[0, 0], schur[0, 0]
    modes = modes[0].transpose(1, 0, 2)
    load = load[0].transpose(1, 0, 2)
    count = count.reshape(1)
    order = order.reshape(1, face)
    scale = scale.reshape(1, face)
    vec, lifted, small = (cases, face), (cases, size), (cases, cases)
    wide0 = up(nc + cases, 128)
    flat0 = up(k * (nc + cases), 128)
    wide1 = up(6 * cases + 3 * PAD, 128)
    wide2 = up((6 + cases // PAD) * cases, 128)
    wide3 = up(8 * cases, 128)
    work = [(nc, cases), (rows + 2 * stride, cases)]
    packet = (up(PAD + cases + 1, 8), face)
    head = functools.partial
    line = {"subs": subs, "chain": chain}
    grid = {"stride": stride, "k": k}

    basis, own, to_even, to_odd, payload = call(
        head(pack_kernel, subs=subs),
        (me, count, modes, order, load, coarse, rhs, scale),
        [((PAD, size), f32), (packet, f32), (packet, f32), (packet, f32), ((peers, 1, flat0), f32)],
        "pack",
        scratch=[modes.shape, pltpu.VMEM(order.shape, jnp.int32), load.shape, coarse.shape, vec, scale.shape],
        scalars=(0, 1),
        far=(2, 3, 4, 5, 6, 7),
        sems=6,
    )
    got = exchange(to_even, to_odd)
    shared = spread(payload)
    high, low = call(
        head(permute_kernel, subs=subs),
        (me, order, schur),
        [((size, size), bf16), ((size, size), bf16)],
        "permute",
    )
    near, coarse_rows = call(
        head(load_kernel, **grid),
        (me, shared),
        [((3 * PAD, cases), f32), ((peers, PAD, wide0), f32)],
        "load",
        scratch=work,
    )
    coarse_rows = coarse_rows.reshape(rows, wide0)

    frame, lifted_rhs, lifted_scale, start, image, to_even, to_odd, payload = call(
        head(start_kernel, **line),
        (me, near, high, low, basis, own, *got),
        [
            ((3 * PAD, size), f32), (lifted, f32), ((1, size), f32), (vec, f32), (lifted, f32),
            (vec, f32), (vec, f32), ((peers, PAD, wide1), f32),
        ],
        "start",
    )
    got = exchange(to_even, to_odd)
    first = spread(payload).reshape(rows, wide1)
    near, _ = call(
        head(project_kernel, total=False, **grid),
        (me, first, first, coarse_rows),
        [((6 * PAD, cases), f32), (small, f32)],
        "project_start",
        scratch=work,
    )

    search, residual, image, to_even, to_odd, payload = call(
        head(direction_kernel, **line),
        (me, near, high, low, frame, lifted_rhs, lifted_scale, image, *got),
        [(lifted, f32), (vec, f32), (lifted, f32), (vec, f32), (vec, f32), ((peers, PAD, wide2), f32)],
        "direction",
    )
    got = exchange(to_even, to_odd)
    shared = spread(payload).reshape(rows, wide2)
    near, curvature = call(
        head(project_kernel, total=True, **grid),
        (me, shared, first, coarse_rows),
        [((6 * PAD, cases), f32), (small, f32)],
        "project_image",
        scratch=work,
    )

    projected, second, image, to_even, to_odd, payload = call(
        head(second_kernel, **line),
        (me, near, high, low, frame, lifted_scale, search, residual, image, *got),
        [(vec, f32), (vec, f32), (vec, f32), (vec, f32), (vec, f32), ((peers, cases, wide3), f32)],
        "second",
    )
    got = exchange(to_even, to_odd)
    shared = spread(payload)
    (inverse,) = call(invert_kernel, (curvature,), [(small, f32)], "invert", scalars=())
    (steps,) = call(
        head(step_kernel, k=k, **line),
        (me, shared, coarse_rows, inverse),
        [((2 * cases + 2 * PAD, cases), f32)],
        "step",
        scratch=[(nc, cases)],
    )
    multipliers, residual = call(
        head(finish_kernel, **line),
        (me, steps, frame, start, search, residual, projected, second, image, *got),
        [(vec, f32), (vec, f32)],
        "finish",
    )
    return multipliers[None, None], residual[None, None]


def solution(mesh):
    in_specs = (
        P("sub", "cluster", None, None),
        P("sub", "cluster", None, None),
        P("sub", "cluster", None, None),
        P("sub", "cluster"),
        P("sub", "cluster", None),
        P("sub", "cluster", None),
        P("sub", "cluster", None, None),
        P(("cluster", "sub"), None),
    )
    out_specs = (P("sub", "cluster", None, None), P("sub", "cluster", None, None))
    return jax.shard_map(shards, mesh=mesh, in_specs=in_specs, out_specs=out_specs, check_vma=False)
```

```python
import functools
import math
import jax
import jax.numpy as jnp
from jax import lax
from jax.experimental import pallas as pl
from jax.experimental.pallas import tpu as pltpu
from jax.sharding import PartitionSpec as P

AXES = ("cluster", "sub")
f32 = jnp.float32
bf16 = jnp.bfloat16
PAD = 8


def dot(a, b, ca, cb):
    return lax.dot_general(
        a, b, (((ca,), (cb,)), ((), ())), precision=lax.Precision.HIGHEST, preferred_element_type=f32
    )


def nn(a, b):
    return dot(a, b, 1, 0)


def nt(a, b):
    return dot(a, b, 1, 1)


def tn(a, b):
    return dot(a, b, 0, 0)


def bdot(a, b, ca, cb):
    return lax.dot_general(a, b, (((ca,), (cb,)), ((), ())), preferred_element_type=f32)


def halves(x):
    high = x.astype(bf16)
    return high, (x - high.astype(f32)).astype(bf16)


def times_schur(x, high_ref, low_ref):
    rows = x.shape[0]
    xh, xl = halves(x)
    both = bdot(jnp.concatenate([xh, xl], axis=0), high_ref[...], 1, 0)
    return both[:rows] + both[rows:] + bdot(xh, low_ref[...], 1, 0)


def permuted_exact(x, one_hot):
    x1 = x.astype(bf16)
    rest = x - x1.astype(f32)
    x2 = rest.astype(bf16)
    x3 = (rest - x2.astype(f32)).astype(bf16)
    return bdot(x1, one_hot, 1, 1) + bdot(x2, one_hot, 1, 1) + bdot(x3, one_hot, 1, 1)


def split_sides(me, subs, right, left):
    even = (me // subs) % 2 == 0
    return jnp.where(even, right, left), jnp.where(even, left, right)


def join_sides(me, subs, chain, even_got, odd_got):
    at = me // subs
    even = at % 2 == 0
    left = jnp.where(even, odd_got, even_got)
    right = jnp.where(even, even_got, odd_got)
    return jnp.where(at > 0, left, 0.0), jnp.where(at < chain - 1, right, 0.0)


def signed_one_hot(me, subs, order):
    face = order.shape[1]
    hit = lax.broadcasted_iota(jnp.int32, (face, face), 0) == order
    sign = jnp.where(me // subs > 0, -1.0, 0.0)
    return jnp.where(hit, sign, 0.0).astype(bf16)


def pack_kernel(
    me, count, modes_in, order_in, load_in, coarse_in, rhs_in, scale_in,
    basis, own, to_even, to_odd, payload,
    modes, order, load, coarse, rhs, scale, sems, *, subs,
):
    pairs = (
        (order_in, order), (modes_in, modes), (coarse_in, coarse), (rhs_in, rhs),
        (scale_in, scale), (load_in, load),
    )
    copies = [pltpu.make_async_copy(a, b, sems.at[i]) for i, (a, b) in enumerate(pairs)]
    for copy in copies:
        copy.start()
    own[...] = jnp.zeros_like(own)
    basis[...] = jnp.zeros_like(basis)
    face = order.shape[1]
    k = modes.shape[0]
    cases = rhs.shape[0]
    nc = coarse.shape[1]
    copies[0].wait()
    one_hot = signed_one_hot(me[0], subs, order[...])
    for copy in copies[1:]:
        copy.wait()
    used = lax.broadcasted_iota(jnp.int32, (k, 1), 0) < count[0]
    for i in range(k):
        basis[i : i + 1] = jnp.where(i < count[0], modes[i], 0.0)
    left = permuted_exact(basis[:, :face], one_hot)
    basis[:, :face] = left
    own[:PAD] = basis[:, face:]
    own[PAD : PAD + cases] = rhs[...]
    own[PAD + cases : PAD + cases + 1] = scale[...]
    rest = jnp.zeros((own.shape[0] - PAD, face), f32)
    to_even[...], to_odd[...] = split_sides(
        me[0], subs, own[...], jnp.concatenate([left, rest], axis=0)
    )
    peers = payload.shape[0]
    each = nc + cases
    line = []
    for i in range(k):
        line = line + [coarse[i : i + 1], jnp.where(i < count[0], load[i], 0.0)]
    line = line + [jnp.zeros((1, payload.shape[2] - k * each), f32)]
    payload[...] = jnp.broadcast_to(jnp.concatenate(line, axis=1)[None], payload.shape)


def permute_kernel(me, order, schur, high, low, *, subs):
    face = order.shape[1]
    one_hot = signed_one_hot(me[0], subs, order[...])
    sh, sl = halves(schur[...])
    for part, out in ((sh, high), (sl, low)):
        top = bdot(one_hot, part[:face], 1, 0).astype(bf16)
        out[:face, :face] = bdot(top[:, :face], one_hot, 1, 1).astype(bf16)
        out[:face, face:] = top[:, face:]
        out[face:, :face] = bdot(part[face:, :face], one_hot, 1, 1).astype(bf16)
        out[face:, face:] = part[face:, face:]


def coarse_times(rows_ref, nc, values, packed, k):
    for i in range(nc // k):
        packed[i * k : (i + 1) * k] = values[i * PAD : i * PAD + k]
    return nn(rows_ref[:, :nc], packed[...])


def near_blocks(values, padded, here, stride):
    rows = values.shape[0]
    padded[:stride] = jnp.zeros((stride, values.shape[1]), f32)
    padded[stride + rows :] = jnp.zeros((stride, values.shape[1]), f32)
    padded[stride : stride + rows] = values
    start = here * PAD
    return jnp.concatenate(
        [padded[pl.ds(pl.multiple_of(start + b * stride, PAD), PAD), :] for b in range(3)], axis=0
    )


def gather_sum(wide, first, cases, stride):
    part = [wide[:, first + b * cases : first + (b + 1) * cases] for b in range(3)]
    none = jnp.zeros((stride, cases), f32)
    return (
        part[1]
        + jnp.concatenate([part[0][stride:], none], axis=0)
        + jnp.concatenate([none, part[2][:-stride]], axis=0)
    )


def scaled_gram_times(wide, first, values, k, near):
    rows, cases = values.shape
    blocks = rows // PAD
    matrix = wide[:, first : first + 3 * PAD].reshape(blocks, PAD, 3 * PAD)
    vector = values.reshape(blocks, PAD, cases)
    none = jnp.zeros((near, PAD, cases), f32)
    moved = [
        jnp.concatenate([none, vector[:-near]], axis=0),
        vector,
        jnp.concatenate([vector[near:], none], axis=0),
    ]
    total = jnp.zeros((blocks, PAD, cases), f32)
    for b in range(3):
        for m in range(k):
            total = total + matrix[:, :, b * PAD + m : b * PAD + m + 1] * moved[b][:, m : m + 1, :]
    return total.reshape(rows, cases)


def side_by_side(tall, blocks):
    return [tall[b * PAD : (b + 1) * PAD] for b in range(blocks)]


def frame_kernel(
    me, high, low, basis, own, even_got, odd_got,
    frame, lifted_rhs, lifted_scale, applied, mine, scaled, *, subs, chain,
):
    face = own.shape[1]
    cases = lifted_rhs.shape[0]
    from_left, from_right = join_sides(me[0], subs, chain, even_got[...], odd_got[...])
    zero = jnp.zeros((PAD, face), f32)
    v = jnp.concatenate(
        [
            jnp.concatenate([from_left[:PAD], zero], axis=1),
            basis[...],
            jnp.concatenate([zero, from_right[:PAD]], axis=1),
        ],
        axis=0,
    )
    both = jnp.concatenate([from_left, own[...]], axis=1)
    lb = both[PAD : PAD + cases]
    ld = both[PAD + cases : PAD + cases + 1]
    frame[: 3 * PAD] = v
    frame[3 * PAD :] = v * ld
    lifted_rhs[...] = lb
    lifted_scale[...] = ld
    applied[...] = times_schur(v, high, low)
    bd = basis[...] * ld
    mine[...] = nt(jnp.concatenate([basis[...], bd], axis=0), lb)
    scaled[...] = nt(bd, v)


def start_kernel(
    me, gathered, frame, applied, mine, scaled,
    start, image_out, to_even, to_odd, rows, payload, packed, padded, *, subs, stride, k,
):
    face = start.shape[1]
    nc, cases = packed.shape
    each = nc + cases
    peers = gathered.shape[0]
    rows[...] = jnp.zeros_like(rows)
    for i in range(k):
        rows[:, i, :each] = gathered[:, 0, i * each : (i + 1) * each]
    for i in range(peers):
        packed[i * k : (i + 1) * k] = rows[i, :k, nc:each]
    table = rows[:, :, :nc].reshape(peers * PAD, nc)
    near = near_blocks(nn(table, packed[...]), padded, me[0], stride)
    start[...] = tn(near, frame[: 3 * PAD, face:])
    image = tn(near, applied[...])
    image_out[...] = image
    to_even[...], to_odd[...] = split_sides(me[0], subs, image[:, face:], image[:, :face])
    part = side_by_side(-nt(frame[...], image), 6)
    part[1] = part[1] + mine[:PAD]
    part[4] = part[4] + mine[PAD:]
    used = 6 * cases + 3 * PAD
    width = payload.shape[2] // k
    row = jnp.concatenate(part + [scaled[...], jnp.zeros((PAD, width - used), f32)], axis=1)
    line = jnp.concatenate([row[i : i + 1] for i in range(k)], axis=1)
    payload[...] = jnp.broadcast_to(line[None], payload.shape)


def project_first_kernel(me, gathered, coarse, near, unfolded, packed, padded, *, stride, k):
    nc, cases = packed.shape
    peers, _, width = unfolded.shape
    unfolded[...] = jnp.zeros_like(unfolded)
    for i in range(k):
        unfolded[:, i, :] = gathered[:, 0, i * width : (i + 1) * width]
    wide = unfolded[...].reshape(peers * PAD, width)
    project(me, wide, wide, coarse, near, packed, padded, nc, cases, stride, k)


def project(me, wide, scaled, coarse, near, packed, padded, nc, cases, stride, k):
    g = gather_sum(wide, 0, cases, stride)
    h = gather_sum(wide, 3 * cases, cases, stride)
    c1 = coarse_times(coarse, nc, g, packed, k)
    c2 = coarse_times(
        coarse, nc, h - scaled_gram_times(scaled, 6 * cases, c1, k, stride // PAD), packed, k
    )
    near[: 3 * PAD] = near_blocks(c1, padded, me[0], stride)
    near[3 * PAD :] = near_blocks(c2, padded, me[0], stride)


def project_kernel(me, gathered, scaled, coarse, near, curvature, packed, padded, *, stride, k):
    nc, cases = packed.shape
    wide = gathered[...]
    project(me, wide, scaled[...], coarse, near, packed, padded, nc, cases, stride, k)
    for b in range(cases // PAD):
        piece = wide[:, (6 + b) * cases : (7 + b) * cases]
        curvature[b * PAD : (b + 1) * PAD] = piece.reshape(-1, PAD, cases).sum(axis=0)


def direction_kernel(
    me, near, high, low, frame, lifted_rhs, lifted_scale, image_in, even_got, odd_got,
    search, residual, image_out, to_even, to_odd, payload, *, subs, chain,
):
    cases, face = even_got.shape
    from_left, from_right = join_sides(me[0], subs, chain, even_got[...], odd_got[...])
    moved = image_in[...] + jnp.concatenate([from_left, from_right], axis=1)
    v = frame[: 3 * PAD]
    r = lifted_rhs[...] - moved - tn(near[: 3 * PAD], v)
    s = lifted_scale[...] * r - tn(near[3 * PAD :], v)
    search[...] = s
    residual[...] = r[:, face:]
    image = times_schur(s, high, low)
    image_out[...] = image
    to_even[...], to_odd[...] = split_sides(me[0], subs, image[:, face:], image[:, :face])
    shares = nt(frame[...], image)
    energy = nt(s, image)
    part = side_by_side(shares, 6) + side_by_side(energy, cases // PAD)
    used = (6 + cases // PAD) * cases
    width = payload.shape[2]
    if width > used:
        part = part + [jnp.zeros((PAD, width - used), f32)]
    payload[...] = jnp.broadcast_to(jnp.concatenate(part, axis=1)[None], payload.shape)


def second_kernel(
    me, near, high, low, frame, lifted_scale, search, residual, image_in, even_got, odd_got,
    projected, second, image_out, to_even, to_odd, payload, *, subs, chain,
):
    cases, face = even_got.shape
    from_left, from_right = join_sides(me[0], subs, chain, even_got[...], odd_got[...])
    q = image_in[...] + jnp.concatenate([from_left, from_right], axis=1)
    v = frame[: 3 * PAD]
    p = q - tn(near[: 3 * PAD], v)
    z = lifted_scale[...] * p - tn(near[3 * PAD :], v)
    projected[...] = p[:, face:]
    zr = z[:, face:]
    second[...] = zr
    image = times_schur(z, high, low)
    image_out[...] = image[:, face:]
    to_even[...], to_odd[...] = split_sides(me[0], subs, image[:, face:], image[:, :face])
    grams = nt(
        jnp.concatenate([search[:, face:], zr, q[:, face:]], axis=0),
        jnp.concatenate([residual[...], p[:, face:], zr], axis=0),
    )
    energy = nt(z, image)
    shares = side_by_side(nt(v, image), 3)
    top, bottom = grams[:cases, : 2 * cases], grams[cases : 2 * cases, : 2 * cases]
    crossed = grams[2 * cases :, 2 * cases :]
    extra_top = jnp.concatenate(shares[:2], axis=1)
    extra_low = jnp.concatenate([shares[2], jnp.zeros((PAD, cases), f32)], axis=1)
    extra = jnp.concatenate([extra_top, extra_low], axis=0)
    row = [top, crossed, bottom, energy, extra]
    used = 8 * cases
    width = payload.shape[2]
    if width > used:
        row = row + [jnp.zeros((cases, width - used), f32)]
    payload[...] = jnp.broadcast_to(jnp.concatenate(row, axis=1)[None], payload.shape)


def eliminate(matrix, right):
    n = matrix.shape[0]
    work = jnp.concatenate([matrix, right], axis=1)
    rows = lax.broadcasted_iota(jnp.int32, work.shape, 0)
    for i in range(n):
        row = work[i : i + 1] / work[i : i + 1, i : i + 1]
        work = jnp.where(rows == i, row, work - work[:, i : i + 1] * row)
    return work[:, n:]


def invert_kernel(curvature, inverse):
    n = curvature.shape[0]
    rows = lax.broadcasted_iota(jnp.int32, (n, n), 0)
    columns = lax.broadcasted_iota(jnp.int32, (n, n), 1)
    inverse[...] = eliminate(curvature[...], jnp.where(rows == columns, 1.0, 0.0))


def step_kernel(me, gathered, coarse, inverse, steps, packed, *, subs, chain, k):
    nc, cases = packed.shape
    all_of = gathered[...]
    peers = all_of.shape[0]
    total = all_of.sum(axis=0)
    sr, sp, qz, zr, zp, zw = [total[:, b * cases : (b + 1) * cases] for b in range(6)]
    low, mid = 6 * cases, 7 * cases
    part = [
        all_of[:, :PAD, low:mid],
        all_of[:, :PAD, mid : mid + cases],
        all_of[:, PAD : 2 * PAD, low:mid],
    ]
    none = jnp.zeros((subs, PAD, cases), f32)
    g = (
        part[1]
        + jnp.concatenate([part[0][subs:], none], axis=0)
        + jnp.concatenate([none, part[2][:-subs]], axis=0)
    ).reshape(peers * PAD, cases)
    for i in range(nc // k):
        packed[i * k : (i + 1) * k] = g[i * PAD : i * PAD + k]
    row = pl.multiple_of(me[0] * PAD, PAD)
    after = pl.multiple_of(jnp.minimum(me[0] + subs, peers - 1) * PAD, PAD)
    rows = jnp.concatenate([coarse[pl.ds(row, PAD), :nc], coarse[pl.ds(after, PAD), :nc]], axis=0)
    own = nn(rows, packed[...])
    solved = nn(inverse[...], jnp.concatenate([sr, qz], axis=1))
    a0, y = solved[:, :cases], solved[:, cases:]
    x = nn(y, a0)
    w1 = tn(a0, nn(zw, a0) - tn(qz, x))
    e1 = tn(x, sr - nn(sp, a0)) - tn(a0, zr - nn(zp, a0))
    a1 = eliminate(w1, e1)
    steps[:cases] = a0 + nn(x, a1)
    steps[cases : 2 * cases] = nn(a0, a1)
    steps[2 * cases :] = own


def finish_kernel(
    me, steps, frame, start, search, residual, projected, second, image, even_got, odd_got,
    out_mult, out_res, *, subs, chain,
):
    cases, face = start.shape
    _, from_right = join_sides(me[0], subs, chain, even_got[...], odd_got[...])
    w = image[...] + from_right - tn(steps[2 * cases :], frame[PAD : 3 * PAD, face:])
    first, last = steps[:cases], steps[cases : 2 * cases]
    out_mult[...] = start[...] + tn(first, search[:, face:]) - tn(last, second[...])
    out_res[...] = residual[...] - tn(first, projected[...]) + tn(last, w)


VMEM = pl.BlockSpec(memory_space=pltpu.VMEM)
SMEM = pl.BlockSpec(memory_space=pltpu.SMEM)
FAR = pl.BlockSpec(memory_space=pltpu.HBM)


def up(value, unit):
    return -(-value // unit) * unit


def call(kernel, args, outs, name, scratch=(), scalars=(0,), far=(), sems=0):
    shapes = [(a.shape, a.dtype) for i, a in enumerate(args) if i not in far + scalars]
    shapes = shapes + list(outs) + [(s, f32) for s in scratch if isinstance(s, tuple)]
    need = sum(math.prod(s[:-1]) * up(s[-1], 128) * jnp.dtype(d).itemsize for s, d in shapes)
    limit = 60 * 1024 * 1024 if far else min(2 * need + (6 << 20), 60 << 20)
    spaces = [SMEM if i in scalars else FAR if i in far else VMEM for i in range(len(args))]
    extra = [pltpu.SemaphoreType.DMA((sems,))] if sems else []
    return pl.pallas_call(
        kernel,
        out_shape=[jax.ShapeDtypeStruct(s, d) for s, d in outs],
        in_specs=spaces,
        out_specs=[VMEM] * len(outs),
        scratch_shapes=[s if not isinstance(s, tuple) else pltpu.VMEM(s, f32) for s in scratch] + extra,
        name=name,
        compiler_params=pltpu.CompilerParams(vmem_limit_bytes=limit),
    )(*args)


def exchange(to_even, to_odd):
    chain = lax.axis_size("cluster")
    subs = lax.axis_size("sub")
    even, odd = [], []
    for c in range(chain):
        for t in range(subs):
            even.append((c * subs + t, (c ^ 1) * subs + t))
            if c in (0, chain - 1):
                odd.append((c * subs + t, c * subs + (t ^ 1)))
            else:
                odd.append((c * subs + t, (((c + 1) ^ 1) - 1) * subs + t))
    return lax.ppermute(to_even, AXES, even), lax.ppermute(to_odd, AXES, odd)


def spread(payload):
    return lax.all_to_all(payload, AXES, 0, 0)


def shards(rhs, schur, modes, count, order, scale, load, coarse):
    chain = lax.axis_size("cluster")
    subs = lax.axis_size("sub")
    peers = chain * subs
    cases, face = rhs.shape[2:]
    size = schur.shape[2]
    k = modes.shape[2]
    nc = coarse.shape[1]
    stride = subs * PAD
    rows = peers * PAD
    me = (lax.axis_index("cluster") * subs + lax.axis_index("sub")).astype(jnp.int32).reshape(1)
    rhs, schur = rhs[0, 0], schur[0, 0]
    modes = modes[0].transpose(1, 0, 2)
    load = load[0].transpose(1, 0, 2)
    count = count.reshape(1)
    order = order.reshape(1, face)
    scale = scale.reshape(1, face)
    vec, lifted, small = (cases, face), (cases, size), (cases, cases)
    wide0 = up(nc + cases, 128)
    flat0 = up(k * (nc + cases), 128)
    wide1 = up(6 * cases + 3 * PAD, 128)
    wide2 = up((6 + cases // PAD) * cases, 128)
    wide3 = up(8 * cases, 128)
    work = [(nc, cases), (rows + 2 * stride, cases)]
    packet = (up(PAD + cases + 1, 8), face)
    head = functools.partial
    line = {"subs": subs, "chain": chain}
    grid = {"stride": stride, "k": k}

    basis, own, to_even, to_odd, payload = call(
        head(pack_kernel, subs=subs),
        (me, count, modes, order, load, coarse, rhs, scale),
        [((PAD, size), f32), (packet, f32), (packet, f32), (packet, f32), ((peers, 1, flat0), f32)],
        "pack",
        scratch=[modes.shape, pltpu.VMEM(order.shape, jnp.int32), load.shape, coarse.shape, vec, scale.shape],
        scalars=(0, 1),
        far=(2, 3, 4, 5, 6, 7),
        sems=6,
    )
    got = exchange(to_even, to_odd)
    shared = spread(payload)
    high, low = call(
        head(permute_kernel, subs=subs),
        (me, order, schur),
        [((size, size), bf16), ((size, size), bf16)],
        "permute",
    )
    frame, lifted_rhs, lifted_scale, applied, mine, scaled = call(
        head(frame_kernel, **line),
        (me, high, low, basis, own, *got),
        [
            ((6 * PAD, size), f32), (lifted, f32), ((1, size), f32), ((3 * PAD, size), f32),
            ((2 * PAD, cases), f32), ((PAD, 3 * PAD), f32),
        ],
        "frame",
    )
    start, image, to_even, to_odd, coarse_rows, payload = call(
        head(start_kernel, subs=subs, **grid),
        (me, shared, frame, applied, mine, scaled),
        [
            (vec, f32), (lifted, f32), (vec, f32), (vec, f32), ((peers, PAD, wide0), f32),
            ((peers, 1, k * wide1), f32),
        ],
        "start",
        scratch=work,
    )
    coarse_rows = coarse_rows.reshape(rows, wide0)
    got = exchange(to_even, to_odd)
    near, first = call(
        head(project_first_kernel, **grid),
        (me, spread(payload), coarse_rows),
        [((6 * PAD, cases), f32), ((peers, PAD, wide1), f32)],
        "project_start",
        scratch=work,
    )
    first = first.reshape(rows, wide1)

    search, residual, image, to_even, to_odd, payload = call(
        head(direction_kernel, **line),
        (me, near, high, low, frame, lifted_rhs, lifted_scale, image, *got),
        [(lifted, f32), (vec, f32), (lifted, f32), (vec, f32), (vec, f32), ((peers, PAD, wide2), f32)],
        "direction",
    )
    got = exchange(to_even, to_odd)
    shared = spread(payload).reshape(rows, wide2)
    near, curvature = call(
        head(project_kernel, **grid),
        (me, shared, first, coarse_rows),
        [((6 * PAD, cases), f32), (small, f32)],
        "project_image",
        scratch=work,
    )

    projected, second, image, to_even, to_odd, payload = call(
        head(second_kernel, **line),
        (me, near, high, low, frame, lifted_scale, search, residual, image, *got),
        [(vec, f32), (vec, f32), (vec, f32), (vec, f32), (vec, f32), ((peers, cases, wide3), f32)],
        "second",
    )
    got = exchange(to_even, to_odd)
    shared = spread(payload)
    (inverse,) = call(invert_kernel, (curvature,), [(small, f32)], "invert", scalars=())
    (steps,) = call(
        head(step_kernel, k=k, **line),
        (me, shared, coarse_rows, inverse),
        [((2 * cases + 2 * PAD, cases), f32)],
        "step",
        scratch=[(nc, cases)],
    )
    multipliers, residual = call(
        head(finish_kernel, **line),
        (me, steps, frame, start, search, residual, projected, second, image, *got),
        [(vec, f32), (vec, f32)],
        "finish",
    )
    return multipliers[None, None], residual[None, None]


def solution(mesh):
    in_specs = (
        P("sub", "cluster", None, None),
        P("sub", "cluster", None, None),
        P("sub", "cluster", None, None),
        P("sub", "cluster"),
        P("sub", "cluster", None),
        P("sub", "cluster", None),
        P("sub", "cluster", None, None),
        P(("cluster", "sub"), None),
    )
    out_specs = (P("sub", "cluster", None, None), P("sub", "cluster", None, None))
    return jax.shard_map(shards, mesh=mesh, in_specs=in_specs, out_specs=out_specs, check_vma=False)
```
